32 devices in a mesh: dp: 4 (over z), tp: 8 (over y, x, core).
Axes of the slice: x: 2, y: 2, z: 4, core: 2. Of those that a mesh axis runs over, the one named last changes fastest.
Arguments:
- hidden: bfloat16 [4, 2048, 3072], P('dp', 'tp'), parts along dimension 0
- norm_attn: float32 [2, 3072], replicated
- w_q: bfloat16 [2, 3072, 24, 128], P(None, None, 'tp')
- w_kv: bfloat16 [2, 3072, 2, 8, 128], replicated
- w_o: bfloat16 [2, 24, 128, 3072], P(None, 'tp')
- norm_mlp: float32 [2, 3072], replicated
- w_gate: bfloat16 [2, 3072, 8192], P(None, None, 'tp')
- w_up: bfloat16 [2, 3072, 8192], P(None, None, 'tp')
- w_down: bfloat16 [2, 8192, 3072], P(None, 'tp')
Outputs:
- output: bfloat16 [4, 2048, 3072], P('dp', 'tp'), parts along dimension 0
There are 4 independent parts. The reference program is written for one: setup_inputs(seed, part) draws one part's arguments, and reference() takes and returns one part's arrays. A program takes and returns all parts, laid end to end along the dimension named above; an argument that names none is the same for every part.
All inputs are finite; a program needn't handle non-finite values.
Results may differ from the reference program's by a relative error of at most 0.0112868.
Values are sent between devices in bfloat16 or wider.
A program may use at most 1 GiB of HBM per device.

```python
import math
import jax
import jax.numpy as jnp
from jax import lax

D = 3072
HEADS = 24
KV_HEADS = 8
HEAD = 128
FF = 8192
BATCH = 1
SEQ = 2048
LAYERS = 2

EPS = 1e-5
ROPE_BASE = 10000.0
GROUP = HEADS // KV_HEADS


def setup_inputs(seed: int = 0, part: int = 0) -> dict:
    root = jax.random.key(seed)
    keys = jax.random.split(root, 9)
    tok_key, scale_key = jax.random.split(jax.random.fold_in(keys[8], part))
    tokens = jax.random.normal(tok_key, (BATCH, SEQ, D), jnp.float32)
    tok_scale = jax.random.uniform(scale_key, (BATCH, SEQ, 1), jnp.float32, 0.5, 2.0)
    hidden = (tokens * tok_scale).astype(jnp.bfloat16)
    qk_gain = math.sqrt(math.sqrt(math.log(max(SEQ / 8.0, 4.0))))
    in_scale = 1.0 / math.sqrt(D)
    out_scale = 1.0 / math.sqrt(HEADS * HEAD)
    ff_scale = 1.0 / math.sqrt(FF)
    norm_attn = 1.0 + 0.3 * jax.random.uniform(keys[0], (LAYERS, D), jnp.float32, -1.0, 1.0)
    w_q = (jax.random.normal(keys[1], (LAYERS, D, HEADS, HEAD), jnp.float32) * (in_scale * qk_gain)).astype(jnp.bfloat16)
    kv_gain = jnp.array([qk_gain, 1.0], jnp.float32).reshape(1, 1, 2, 1, 1)
    w_kv = (jax.random.normal(keys[2], (LAYERS, D, 2, KV_HEADS, HEAD), jnp.float32) * in_scale * kv_gain).astype(jnp.bfloat16)
    w_o = (jax.random.normal(keys[3], (LAYERS, HEADS, HEAD, D), jnp.float32) * out_scale).astype(jnp.bfloat16)
    norm_mlp = 1.0 + 0.3 * jax.random.uniform(keys[4], (LAYERS, D), jnp.float32, -1.0, 1.0)
    w_gate = (jax.random.normal(keys[5], (LAYERS, D, FF), jnp.float32) * in_scale).astype(jnp.bfloat16)
    w_up = (jax.random.normal(keys[6], (LAYERS, D, FF), jnp.float32) * in_scale).astype(jnp.bfloat16)
    w_down = (jax.random.normal(keys[7], (LAYERS, FF, D), jnp.float32) * ff_scale).astype(jnp.bfloat16)
    return {'hidden': hidden, 'norm_attn': norm_attn, 'w_q': w_q, 'w_kv': w_kv, 'w_o': w_o, 'norm_mlp': norm_mlp, 'w_gate': w_gate, 'w_up': w_up, 'w_down': w_down}


def rms_norm(resid, gain):
    mean_sq = jnp.mean(resid * resid, axis=-1, keepdims=True)
    return (resid * lax.rsqrt(mean_sq + EPS) * gain).astype(jnp.bfloat16)


def rope_tables(positions, head_dim):
    half_dim = head_dim // 2
    inv_freq = jnp.power(ROPE_BASE, -2.0 * jnp.arange(half_dim, dtype=jnp.float32) / head_dim)
    angles = positions.astype(jnp.float32)[:, None] * inv_freq[None, :]
    return jnp.cos(angles), jnp.sin(angles)


def apply_rope(proj, cos_t, sin_t):
    half_dim = proj.shape[-1] // 2
    first_half = proj[..., :half_dim]
    second_half = proj[..., half_dim:]
    cos_b = cos_t[:, None, :]
    sin_b = sin_t[:, None, :]
    return jnp.concatenate([first_half * cos_b - second_half * sin_b, second_half * cos_b + first_half * sin_b], axis=-1)


def decoder_layer(resid, layer_w, cos_t, sin_t, causal_mask):
    attn_gain, q_weight, kv_weight, o_weight, mlp_gain, gate_weight, up_weight, down_weight = layer_w
    normed = rms_norm(resid, attn_gain)
    q_proj = jnp.dot(normed, q_weight.reshape(D, HEADS * HEAD), preferred_element_type=jnp.float32).reshape(SEQ, HEADS, HEAD)
    kv_proj = jnp.dot(normed, kv_weight.reshape(D, 2 * KV_HEADS * HEAD), preferred_element_type=jnp.float32).reshape(SEQ, 2, KV_HEADS, HEAD)
    queries = apply_rope(q_proj, cos_t, sin_t).astype(jnp.bfloat16)
    keys = apply_rope(kv_proj[:, 0], cos_t, sin_t).astype(jnp.bfloat16)
    values = kv_proj[:, 1].astype(jnp.bfloat16)
    q_heads = jnp.transpose(queries, (1, 0, 2))
    k_heads = jnp.repeat(jnp.transpose(keys, (1, 0, 2)), GROUP, axis=0)
    v_heads = jnp.repeat(jnp.transpose(values, (1, 0, 2)), GROUP, axis=0)
    inv_sqrt = 1.0 / math.sqrt(HEAD)

    def attend(head_args):
        q_one, k_one, v_one = head_args
        scores = jnp.dot(q_one, k_one.T, preferred_element_type=jnp.float32) * inv_sqrt
        scores = jnp.where(causal_mask, scores, -jnp.inf)
        attn_probs = jax.nn.softmax(scores, axis=-1).astype(jnp.bfloat16)
        return jnp.dot(attn_probs, v_one, preferred_element_type=jnp.float32).astype(jnp.bfloat16)

    context = lax.map(attend, (q_heads, k_heads, v_heads))
    context = jnp.transpose(context, (1, 0, 2)).reshape(SEQ, HEADS * HEAD)
    resid = resid + jnp.dot(context, o_weight.reshape(HEADS * HEAD, D), preferred_element_type=jnp.float32)
    normed = rms_norm(resid, mlp_gain)
    gate_proj = jnp.dot(normed, gate_weight, preferred_element_type=jnp.float32)
    up_proj = jnp.dot(normed, up_weight, preferred_element_type=jnp.float32)
    activated = (jax.nn.silu(gate_proj) * up_proj).astype(jnp.bfloat16)
    return resid + jnp.dot(activated, down_weight, preferred_element_type=jnp.float32)


def reference(hidden, norm_attn, w_q, w_kv, w_o, norm_mlp, w_gate, w_up, w_down):
    positions = jnp.arange(SEQ)
    cos_t, sin_t = rope_tables(positions, HEAD)
    causal_mask = positions[:, None] >= positions[None, :]
    stacked = (norm_attn, w_q, w_kv, w_o, norm_mlp, w_gate, w_up, w_down)

    def one_sequence(seq_tokens):
        def layer_step(resid, layer_w):
            return decoder_layer(resid, layer_w, cos_t, sin_t, causal_mask), None
        final, _ = lax.scan(layer_step, seq_tokens.astype(jnp.float32), stacked)
        return final.astype(jnp.bfloat16)

    return lax.map(one_sequence, hidden)
```

```python
import functools
import math
import jax
import jax.numpy as jnp
from jax import lax
from jax.experimental import pallas as pl
from jax.experimental.pallas import tpu as pltpu
from jax.sharding import PartitionSpec as P

EPS = 1e-5
ROPE_BASE = 10000.0
MESH = pl.DeviceIdType.MESH
VMEM_LIMIT = 67043328
F32 = jnp.float32
BF16 = jnp.bfloat16
N_COPIES = 20


def dot(a, b):
    return jnp.dot(a, b, preferred_element_type=F32)


def places():
    me = lax.axis_index('tp')
    core = lax.rem(me, 2)
    x = lax.rem(lax.div(me, 2), 2)
    y = lax.div(me, 4)
    dx = 2 - 4 * x
    dy = 4 - 8 * y
    return me, me + 1 - 2 * core, dx, dy


def greet(pa, xn, yn):
    barrier = pltpu.get_barrier_semaphore()
    for dev in (pa, xn, yn):
        pl.semaphore_signal(barrier, inc=1, device_id={'tp': dev}, device_id_type=MESH)
    pl.semaphore_wait(barrier, 3)


def make_copies(G, PR, RX, RY, RD, S, ss, rs, pa, xn, yn):
    half = G.shape[1] // 2
    lo, hi = pl.ds(0, half), pl.ds(half, half)
    table = {
        'd1': (G.at[0], G.at[1], pa),
        'xh0': (G.at[0, lo], G.at[3, lo], xn),
        'yh1': (G.at[0, hi], G.at[3, hi], yn),
        'xf': (G.at[3, hi], G.at[5, hi], xn),
        'yf': (G.at[3, lo], G.at[5, lo], yn),
        'xh1': (G.at[0, hi], G.at[7, lo], xn),
        'yh0': (G.at[0, lo], G.at[7, hi], yn),
        'd2': (G.at[3], G.at[2], pa),
        'd4': (G.at[5], G.at[4], pa),
        'd6': (G.at[7], G.at[6], pa),
        'p1': (G.at[1], PR.at[0], pa),
        'p2': (G.at[2], PR.at[1], pa),
        'p4': (G.at[4], PR.at[2], pa),
        'p6': (G.at[6], PR.at[3], pa),
        'X0': (S.at[0, lo], RX.at[lo], xn),
        'Y1': (S.at[0, hi], RY.at[hi], yn),
        'D0': (S.at[1, lo], RD.at[hi], xn),
        'D1': (S.at[1, hi], RD.at[lo], yn),
        'X1': (S.at[2, lo], RX.at[hi], xn),
        'Y0': (S.at[2, hi], RY.at[lo], yn),
    }
    copies = {}
    for i, (name, (src, dst, dev)) in enumerate(table.items()):
        copies[name] = pltpu.make_async_remote_copy(
            src_ref=src, dst_ref=dst, send_sem=ss.at[i], recv_sem=rs.at[i],
            device_id={'tp': dev}, device_id_type=MESH)
    return copies


def start(copies, *names):
    for name in names:
        copies[name].start()


def arrived(copies, *names):
    for name in names:
        copies[name].wait_recv()


def norm_rows(r_ref, g_ref, G):
    rows = r_ref.shape[0]
    step = 32

    @pl.loop(0, rows // step)
    def _(i):
        at = pl.ds(pl.multiple_of(i * step, step), step)
        x = r_ref[at, :].astype(F32)
        mean_sq = jnp.mean(x * x, axis=-1, keepdims=True)
        G[0, at, :] = (x * lax.rsqrt(mean_sq + EPS) * g_ref[...]).astype(BF16)


def finish(copies, r_ref, acc0, PR, RX, RY, o_ref):
    arrived(copies, 'p1', 'X0', 'X1', 'Y0', 'Y1')
    rows = r_ref.shape[0]
    step = 32

    @pl.loop(0, rows // step)
    def _(i):
        at = pl.ds(pl.multiple_of(i * step, step), step)
        total = acc0[at, :] + PR[0, at, :].astype(F32)
        total += RX[at, :].astype(F32) + RY[at, :].astype(F32)
        o_ref[at, :] = (r_ref[at, :].astype(F32) + total).astype(o_ref.dtype)

    for copy in copies.values():
        copy.wait_send()


def project(a_ref, w_ref, width, emit):
    @pl.loop(0, w_ref.shape[1] // width)
    def _(n):
        cols = pl.ds(pl.multiple_of(n * width, width), width)
        emit(cols, dot(a_ref[...], w_ref[:, cols]))


def merge_last(copies, acc7, RD, S):
    arrived(copies, 'D0', 'D1')
    rows = acc7.shape[0]
    step = 32

    @pl.loop(0, rows // step)
    def _(i):
        at = pl.ds(pl.multiple_of(i * step, step), step)
        S[2, at, :] = (acc7[at, :] + RD[at, :].astype(F32)).astype(BF16)

    start(copies, 'X1', 'Y0')


def emitters(G, PR, S, acc0, acc7):
    def to_partner(j):
        def emit(cols, part):
            G[j, :, cols] = part.astype(BF16)
        return emit

    def chip_sum(i, slot):
        def emit(cols, part):
            S[slot, :, cols] = (part + PR[i, :, cols].astype(F32)).astype(BF16)
        return emit

    def own(cols, part):
        acc0[:, cols] = part

    def last(cols, part):
        acc7[:, cols] = part + PR[3, :, cols].astype(F32)

    return to_partner, chip_sum, own, last


def mlp_kernel(layer, r_ref, g_ref, wg_h, wu_h, wd_h, o_ref,
               wg, wu, wd, G, PR, RX, RY, RD, S, acc0, acc7, u, ss, rs, ls):
    me, pa, dx, dy = places()
    xn, yn = me + dx, me + dy
    loads = [pltpu.make_async_copy(h.at[layer], v, ls.at[i])
             for i, (h, v) in enumerate(((wg_h, wg), (wu_h, wu), (wd_h, wd)))]
    for load in loads:
        load.start()
    norm_rows(r_ref, g_ref, G)
    greet(pa, xn, yn)
    copies = make_copies(G, PR, RX, RY, RD, S, ss, rs, pa, xn, yn)
    to_partner, chip_sum, own, last = emitters(G, PR, S, acc0, acc7)
    start(copies, 'xh0', 'yh1', 'd1')

    def hidden(j):
        width = 256

        @pl.loop(0, wg.shape[1] // width)
        def _(n):
            cols = pl.ds(pl.multiple_of(n * width, width), width)
            gate = dot(G[j], wg[:, cols])
            up = dot(G[j], wu[:, cols])
            u[:, cols] = (jax.nn.silu(gate) * up).astype(BF16)

    def tile(j, emit):
        hidden(j)
        project(u, wd, 512, emit)

    for load in loads:
        load.wait()
    tile(0, own)
    arrived(copies, 'd1')
    tile(1, to_partner(1))
    start(copies, 'p1')
    arrived(copies, 'xh0', 'yh1')
    start(copies, 'xf', 'yf', 'd2', 'xh1', 'yh0')
    arrived(copies, 'd2')
    tile(2, to_partner(2))
    start(copies, 'p2')
    arrived(copies, 'p2')
    tile(3, chip_sum(1, 0))
    start(copies, 'X0', 'Y1')
    arrived(copies, 'xf', 'yf')
    start(copies, 'd4')
    arrived(copies, 'd4')
    tile(4, to_partner(4))
    start(copies, 'p4')
    arrived(copies, 'p4')
    tile(5, chip_sum(2, 1))
    start(copies, 'D0', 'D1')
    arrived(copies, 'xh1', 'yh0')
    start(copies, 'd6')
    arrived(copies, 'd6')
    tile(6, to_partner(6))
    start(copies, 'p6')
    arrived(copies, 'p6')
    tile(7, last)
    merge_last(copies, acc7, RD, S)
    finish(copies, r_ref, acc0, PR, RX, RY, o_ref)


def attn_kernel(layer, head_dim, r_ref, g_ref, cos_ref, sin_ref, wqkv_h, wo_h, o_ref,
                wqkv, wo, G, PR, RX, RY, RD, S, acc0, acc7, q_s, k_s, v_s, sc, l_s, ctx_acc, c_s, ss, rs, ls):
    me, pa, dx, dy = places()
    xn, yn = me + dx, me + dy
    loads = [pltpu.make_async_copy(h.at[layer], v, ls.at[i])
             for i, (h, v) in enumerate(((wqkv_h, wqkv), (wo_h, wo)))]
    for load in loads:
        load.start()
    norm_rows(r_ref, g_ref, G)
    greet(pa, xn, yn)
    copies = make_copies(G, PR, RX, RY, RD, S, ss, rs, pa, xn, yn)
    to_partner, chip_sum, own, last = emitters(G, PR, S, acc0, acc7)
    start(copies, 'xh0', 'yh1', 'd1')

    rows = r_ref.shape[0]
    half = rows // 2
    hd = head_dim
    group = wo.shape[0] // hd
    chunk = sc.shape[2]

    def halves(j):
        dev = me if j in (0, 3, 5, 7) else pa
        if j in (0, 1):
            first, second = dev, dev
        elif j in (4, 5):
            first = second = dev + dx + dy
        else:
            first, second = dev + dx, dev + dy
        if j in (6, 7):
            return first * rows + half, second * rows
        return first * rows, second * rows + half

    def qkv(j):
        for hh, pos in enumerate(halves(j)):
            pos = pl.multiple_of(pos, half)
            at = pl.ds(pos, half)
            proj = dot(G[j, hh * half:(hh + 1) * half, :], wqkv[...])
            cos_b = cos_ref[at, :]
            sin_b = sin_ref[at, :]

            def rope(n):
                part = proj[:, n * hd:(n + 1) * hd]
                return (part * cos_b + pltpu.roll(part, hd // 2, 1) * sin_b).astype(BF16)

            slot = lax.div(pos, half)
            for h in range(group):
                q_s[slot, h * half:(h + 1) * half, :] = rope(h)
            k_s[at, :] = rope(group)
            v_s[at, :] = proj[:, (group + 1) * hd:].astype(BF16)

    scale = math.log2(math.e) / math.sqrt(hd)

    def scores(q, start_key):
        keys = k_s[pl.ds(start_key, chunk), :]
        return lax.dot_general(q, keys, (((1,), (1,)), ((), ())), preferred_element_type=F32)

    def fold(s, op):
        out = s[:, :hd]
        for n in range(1, chunk // hd):
            out = op(out, s[:, n * hd:(n + 1) * hd])
        return out

    def attend(pos, out_row):
        q = q_s[lax.div(pos, half)]
        n_full = lax.div(pos, chunk)
        edge = pl.multiple_of(n_full * chunk, chunk)
        s = scores(q, edge)
        shape = (half, chunk)
        row = lax.broadcasted_iota(jnp.int32, shape, 0) + (pos - edge)
        keep = lax.broadcasted_iota(jnp.int32, shape, 1) <= row
        keep = jnp.concatenate([keep] * group, axis=0)
        s = jnp.where(keep, s, -jnp.inf)
        sc[n_full] = s
        l_s[...] = fold(s, jnp.maximum)

        @pl.loop(0, n_full)
        def _(c):
            s = scores(q, pl.multiple_of(c * chunk, chunk))
            sc[c] = s
            l_s[...] = jnp.maximum(l_s[...], fold(s, jnp.maximum))

        top = jnp.max(l_s[...], axis=1, keepdims=True)
        l_s[...] = jnp.zeros_like(l_s)
        ctx_acc[...] = jnp.zeros_like(ctx_acc)

        @pl.loop(0, n_full + 1)
        def _(c):
            p = jnp.exp2((sc[c] - top) * scale)
            l_s[...] += fold(p, jnp.add)
            ctx_acc[...] += dot(p.astype(BF16), v_s[pl.ds(pl.multiple_of(c * chunk, chunk), chunk), :])

        out = (ctx_acc[...] / jnp.sum(l_s[...], axis=1, keepdims=True)).astype(BF16)
        for h in range(group):
            c_s[pl.ds(out_row, half), h * hd:(h + 1) * hd] = out[h * half:(h + 1) * half, :]

    def tile(j, emit):
        first, second = halves(j)

        @pl.loop(0, 2)
        def _(hh):
            attend(pl.multiple_of(first + hh * (second - first), half), pl.multiple_of(hh * half, half))

        project(c_s, wo, 512, emit)

    loads[0].wait()
    qkv(0)
    arrived(copies, 'd1')
    qkv(1)
    arrived(copies, 'xh0', 'yh1')
    start(copies, 'xf', 'yf', 'd2', 'xh1', 'yh0')
    qkv(3)
    arrived(copies, 'd2')
    qkv(2)
    arrived(copies, 'xf', 'yf')
    start(copies, 'd4')
    qkv(5)
    arrived(copies, 'd4')
    qkv(4)
    arrived(copies, 'xh1', 'yh0')
    start(copies, 'd6')
    qkv(7)
    arrived(copies, 'd6')
    qkv(6)
    loads[1].wait()

    tile(4, to_partner(4))
    start(copies, 'p4')
    arrived(copies, 'p4')
    tile(5, chip_sum(2, 1))
    start(copies, 'D0', 'D1')
    tile(2, to_partner(2))
    start(copies, 'p2')
    arrived(copies, 'p2')
    tile(3, chip_sum(1, 0))
    start(copies, 'X0', 'Y1')
    tile(6, to_partner(6))
    start(copies, 'p6')
    arrived(copies, 'p6')
    tile(7, last)
    merge_last(copies, acc7, RD, S)
    tile(1, to_partner(1))
    start(copies, 'p1')
    tile(0, own)
    finish(copies, r_ref, acc0, PR, RX, RY, o_ref)


def comm_scratch(rows, width):
    return [
        pltpu.VMEM((8, rows, width), BF16),
        pltpu.VMEM((4, rows, width), BF16),
        pltpu.VMEM((rows, width), BF16),
        pltpu.VMEM((rows, width), BF16),
        pltpu.VMEM((rows, width), BF16),
        pltpu.VMEM((3, rows, width), BF16),
        pltpu.VMEM((rows, width), F32),
        pltpu.VMEM((rows, width), F32),
    ]


def semaphores(n_loads):
    return [pltpu.SemaphoreType.DMA((N_COPIES,)), pltpu.SemaphoreType.DMA((N_COPIES,)),
            pltpu.SemaphoreType.DMA((n_loads,))]


def call(kernel, collective, out_dtype, rows, width, n_vmem, n_any, scratch, name):
    vmem = pl.BlockSpec(memory_space=pltpu.VMEM)
    return pl.pallas_call(
        kernel,
        out_shape=jax.ShapeDtypeStruct((rows, width), out_dtype),
        in_specs=[vmem] * n_vmem + [pl.BlockSpec(memory_space=pl.ANY)] * n_any,
        out_specs=vmem,
        scratch_shapes=scratch,
        compiler_params=pltpu.CompilerParams(
            collective_id=collective, has_side_effects=True, vmem_limit_bytes=VMEM_LIMIT),
        name=name,
    )


def rope_tables(seq_len, head_dim):
    half_dim = head_dim // 2
    inv_freq = jnp.power(ROPE_BASE, -2.0 * jnp.arange(half_dim, dtype=F32) / head_dim)
    angles = jnp.arange(seq_len).astype(F32)[:, None] * inv_freq[None, :]
    cos_t, sin_t = jnp.cos(angles), jnp.sin(angles)
    return jnp.concatenate([cos_t, cos_t], axis=1), jnp.concatenate([-sin_t, sin_t], axis=1)


def solution(mesh):
    n_tp = mesh.shape['tp']
    tok_spec = P('dp', 'tp', None)
    in_specs = (tok_spec, P(), P(None, None, 'tp', None), P(), P(None, 'tp', None, None), P(), P(None, None, 'tp'), P(None, None, 'tp'), P(None, 'tp', None))

    def body(hidden, norm_attn, w_q, w_kv, w_o, norm_mlp, w_gate, w_up, w_down):
        n_layers, width, heads_loc, hd = w_q.shape
        rows = hidden.shape[1]
        seq_len = rows * n_tp
        half = rows // 2
        ff = w_gate.shape[2]
        chunk = 256
        head = lax.axis_index('tp')
        kv = lax.dynamic_slice_in_dim(w_kv, head, 1, axis=3).reshape(n_layers, width, 2 * hd)
        wqkv = jnp.concatenate([w_q.reshape(n_layers, width, heads_loc * hd), kv], axis=2)
        wo = w_o.reshape(n_layers, heads_loc * hd, width)
        cos_t, sin_t = rope_tables(seq_len, hd)
        attn_scratch = [
            pltpu.VMEM(wqkv.shape[1:], BF16), pltpu.VMEM(wo.shape[1:], BF16), *comm_scratch(rows, width),
            pltpu.VMEM((seq_len // half, heads_loc * half, hd), BF16),
            pltpu.VMEM((seq_len, hd), BF16), pltpu.VMEM((seq_len, hd), BF16),
            pltpu.VMEM((seq_len // chunk, heads_loc * half, chunk), F32),
            pltpu.VMEM((heads_loc * half, hd), F32), pltpu.VMEM((heads_loc * half, hd), F32),
            pltpu.VMEM((rows, heads_loc * hd), BF16), *semaphores(2)]
        mlp_scratch = [
            pltpu.VMEM((width, ff), BF16), pltpu.VMEM((width, ff), BF16), pltpu.VMEM((ff, width), BF16),
            *comm_scratch(rows, width), pltpu.VMEM((rows, ff), BF16), *semaphores(3)]
        resid = hidden[0]
        for layer in range(n_layers):
            out_dtype = BF16 if layer == n_layers - 1 else F32
            resid = call(functools.partial(attn_kernel, layer, hd), 2 * layer, F32, rows, width, 4, 2, attn_scratch, f'attn{layer}')(
                resid, norm_attn[layer][None, :], cos_t, sin_t, wqkv, wo)
            resid = call(functools.partial(mlp_kernel, layer), 2 * layer + 1, out_dtype, rows, width, 2, 3, mlp_scratch, f'mlp{layer}')(
                resid, norm_mlp[layer][None, :], w_gate, w_up, w_down)
        return resid[None]

    return jax.shard_map(body, mesh=mesh, in_specs=in_specs, out_specs=tok_spec, check_vma=False)
```

```python
import functools
import math
import jax
import numpy as np
import jax.numpy as jnp
from jax import lax
from jax.experimental import pallas as pl
from jax.experimental.pallas import tpu as pltpu
from jax.sharding import PartitionSpec as P

EPS = 1e-5
ROPE_BASE = 10000.0
MESH = pl.DeviceIdType.MESH
VMEM_LIMIT = 67043328
F32 = jnp.float32
BF16 = jnp.bfloat16
N_COPIES = 20


def dot(a, b):
    return jnp.dot(a, b, preferred_element_type=F32)


def places():
    me = lax.axis_index('tp')
    core = lax.rem(me, 2)
    x = lax.rem(lax.div(me, 2), 2)
    y = lax.div(me, 4)
    dx = 2 - 4 * x
    dy = 4 - 8 * y
    return me, me + 1 - 2 * core, dx, dy


def greet(pa, xn, yn):
    for dev in (pa, xn, yn):
        pl.semaphore_signal(pltpu.get_barrier_semaphore(), inc=1, device_id={'tp': dev}, device_id_type=MESH)


def all_entered():
    pl.semaphore_wait(pltpu.get_barrier_semaphore(), 3)


def make_copies(G, PR, RX, RY, RD, S, ss, rs, pa, xn, yn):
    half = G.shape[1] // 2
    lo, hi = pl.ds(0, half), pl.ds(half, half)
    table = {
        'd1': (G.at[0], G.at[1], pa),
        'xh0': (G.at[0, lo], G.at[3, lo], xn),
        'yh1': (G.at[0, hi], G.at[3, hi], yn),
        'xf': (G.at[3, hi], G.at[5, hi], xn),
        'yf': (G.at[3, lo], G.at[5, lo], yn),
        'xh1': (G.at[0, hi], G.at[7, lo], xn),
        'yh0': (G.at[0, lo], G.at[7, hi], yn),
        'd2': (G.at[3], G.at[2], pa),
        'd4': (G.at[5], G.at[4], pa),
        'd6': (G.at[7], G.at[6], pa),
        'p1': (G.at[1], PR.at[0], pa),
        'p2': (G.at[2], PR.at[1], pa),
        'p4': (G.at[4], PR.at[2], pa),
        'p6': (G.at[6], PR.at[3], pa),
        'X0': (S.at[0, lo], RX.at[lo], xn),
        'Y1': (S.at[0, hi], RY.at[hi], yn),
        'D0': (S.at[1, lo], RD.at[hi], xn),
        'D1': (S.at[1, hi], RD.at[lo], yn),
        'X1': (S.at[2, lo], RX.at[hi], xn),
        'Y0': (S.at[2, hi], RY.at[lo], yn),
    }
    copies = {}
    for i, (name, (src, dst, dev)) in enumerate(table.items()):
        copies[name] = pltpu.make_async_remote_copy(
            src_ref=src, dst_ref=dst, send_sem=ss.at[i], recv_sem=rs.at[i],
            device_id={'tp': dev}, device_id_type=MESH)
    return copies


def start(copies, *names):
    for name in names:
        copies[name].start()


def arrived(copies, *names):
    for name in names:
        copies[name].wait_recv()


def norm_rows(layer, r_ref, g_ref, G):
    rows = r_ref.shape[0]
    step = 32

    @pl.loop(0, rows // step)
    def _(i):
        at = pl.ds(pl.multiple_of(i * step, step), step)
        x = r_ref[at, :].astype(F32)
        mean_sq = jnp.mean(x * x, axis=-1, keepdims=True)
        G[0, at, :] = (x * lax.rsqrt(mean_sq + EPS) * g_ref[layer:layer + 1, :]).astype(BF16)


def finish(copies, r_ref, acc0, PR, RX, RY, o_ref):
    arrived(copies, 'p1', 'X0', 'X1', 'Y0', 'Y1')
    rows = r_ref.shape[0]
    step = 32

    @pl.loop(0, rows // step)
    def _(i):
        at = pl.ds(pl.multiple_of(i * step, step), step)
        total = acc0[at, :] + PR[0, at, :].astype(F32)
        total += RX[at, :].astype(F32) + RY[at, :].astype(F32)
        o_ref[at, :] = (r_ref[at, :].astype(F32) + total).astype(o_ref.dtype)

    for copy in copies.values():
        copy.wait_send()


def project(a_ref, w_ref, width, emit):
    @pl.loop(0, w_ref.shape[1] // width)
    def _(n):
        cols = pl.ds(pl.multiple_of(n * width, width), width)
        emit(cols, dot(a_ref[...], w_ref[:, cols]))


def merge_last(copies, acc7, RD, S):
    arrived(copies, 'D0', 'D1')
    rows = acc7.shape[0]
    step = 32

    @pl.loop(0, rows // step)
    def _(i):
        at = pl.ds(pl.multiple_of(i * step, step), step)
        S[2, at, :] = (acc7[at, :] + RD[at, :].astype(F32)).astype(BF16)

    start(copies, 'X1', 'Y0')


def emitters(G, PR, S, acc0, acc7):
    def to_partner(j):
        def emit(cols, part):
            G[j, :, cols] = part.astype(BF16)
        return emit

    def chip_sum(i, slot):
        def emit(cols, part):
            S[slot, :, cols] = (part + PR[i, :, cols].astype(F32)).astype(BF16)
        return emit

    def own(cols, part):
        acc0[:, cols] = part

    def last(cols, part):
        acc7[:, cols] = part + PR[3, :, cols].astype(F32)

    return to_partner, chip_sum, own, last


def mlp_kernel(layer, r_ref, g_ref, wg_h, wu_h, wd_h, o_ref,
               wg, wu, wd, G, PR, RX, RY, RD, S, acc0, acc7, u, ss, rs, ls):
    me, pa, dx, dy = places()
    xn, yn = me + dx, me + dy
    greet(pa, xn, yn)
    loads = [pltpu.make_async_copy(h.at[layer], v, ls.at[i])
             for i, (h, v) in enumerate(((wg_h, wg), (wu_h, wu), (wd_h, wd)))]
    for load in loads:
        load.start()
    norm_rows(layer, r_ref, g_ref, G)
    all_entered()
    copies = make_copies(G, PR, RX, RY, RD, S, ss, rs, pa, xn, yn)
    to_partner, chip_sum, own, last = emitters(G, PR, S, acc0, acc7)
    start(copies, 'xh0', 'yh1', 'd1')

    def hidden(j):
        width = 256
        blocks = wg.shape[1] // width

        @pl.loop(0, 2 * blocks)
        def _(i):
            t = lax.div(i, blocks)
            cols = pl.ds(pl.multiple_of(lax.rem(i, blocks) * width, width), width)
            gate = dot(G[j + t], wg[:, cols])
            up = dot(G[j + t], wu[:, cols])
            u[t, :, cols] = (jax.nn.silu(gate) * up).astype(BF16)

    def down(t, emit):
        project(u.at[t], wd, 512, emit)

    for load in loads:
        load.wait()
    arrived(copies, 'd1')
    hidden(0)
    down(1, to_partner(1))
    start(copies, 'p1')
    arrived(copies, 'xh0', 'yh1')
    start(copies, 'xf', 'yf', 'd2', 'xh1', 'yh0')
    down(0, own)
    arrived(copies, 'd2')
    hidden(2)
    down(0, to_partner(2))
    start(copies, 'p2')
    arrived(copies, 'p2')
    down(1, chip_sum(1, 0))
    start(copies, 'X0', 'Y1')
    arrived(copies, 'xf', 'yf')
    start(copies, 'd4')
    arrived(copies, 'd4')
    hidden(4)
    down(0, to_partner(4))
    start(copies, 'p4')
    arrived(copies, 'p4')
    down(1, chip_sum(2, 1))
    start(copies, 'D0', 'D1')
    arrived(copies, 'xh1', 'yh0')
    start(copies, 'd6')
    arrived(copies, 'd6')
    hidden(6)
    down(0, to_partner(6))
    start(copies, 'p6')
    arrived(copies, 'p6')
    down(1, last)
    merge_last(copies, acc7, RD, S)
    finish(copies, r_ref, acc0, PR, RX, RY, o_ref)


def attn_kernel(layer, hd, n_kv, r_ref, g_ref, tab_ref, wq_h, wkv_h, wo_h, o_ref,
                wqkv, wo, G, PR, RX, RY, RD, S, acc0, acc7, q_s, k_s, v_s, sc, l_s, ctx_acc, c_s,
                proj, kv_in, kv_f, ss, rs, ls):
    me, pa, dx, dy = places()
    xn, yn = me + dx, me + dy
    greet(pa, xn, yn)
    rows = r_ref.shape[0]
    half = rows // 2
    group = wo.shape[0] // hd
    chunk = sc.shape[2]
    n_slots = q_s.shape[0]
    kv_rows = kv_in.shape[1]
    depth = kv_rows // (2 * n_kv)
    n_parts = wqkv.shape[0] // depth

    def kv_load(i, slot):
        at = pl.ds(pl.multiple_of(i * kv_rows, kv_rows), kv_rows)
        return pltpu.make_async_copy(wkv_h.at[layer, at], kv_in.at[slot], ls.at[slot])

    kv_load(0, 0).start()
    loads = [pltpu.make_async_copy(wq_h.at[layer, h], wqkv.at[:, h * hd:(h + 1) * hd], ls.at[3 + h])
             for h in range(group)]
    loads.append(pltpu.make_async_copy(wo_h.at[layer], wo, ls.at[2]))
    for load in loads:
        load.start()
    norm_rows(layer, r_ref, g_ref, G)
    all_entered()
    copies = make_copies(G, PR, RX, RY, RD, S, ss, rs, pa, xn, yn)
    to_partner, chip_sum, own, last = emitters(G, PR, S, acc0, acc7)
    start(copies, 'xh0', 'yh1', 'd1')

    @pl.loop(0, n_parts)
    def _(i):
        slot = lax.rem(i, 2)

        @pl.when(i + 1 < n_parts)
        def _():
            kv_load(i + 1, 1 - slot).start()

        kv_load(i, slot).wait()
        piece = 512

        @pl.loop(0, kv_rows // piece)
        def _(n):
            at = pl.ds(pl.multiple_of(n * piece, piece), piece)
            kv_f[at, :] = kv_in[slot, at, :].astype(F32)

        at = pl.ds(pl.multiple_of(i * depth, depth), depth)
        for c in range(2):
            picked = kv_f[pl.ds(me + c * n_kv, depth, stride=2 * n_kv), :]
            wqkv[at, (group + c) * hd:(group + c + 1) * hd] = picked.astype(BF16)

    def halves(j):
        dev = me if j in (0, 3, 5, 7) else pa
        if j in (0, 1):
            first, second = dev, dev
        elif j in (4, 5):
            first = second = dev + dx + dy
        else:
            first, second = dev + dx, dev + dy
        if j in (6, 7):
            return first * rows + half, second * rows
        return first * rows, second * rows + half

    def qkv(j):
        proj[...] = dot(G[j], wqkv[...])
        first, second = halves(j)

        @pl.loop(0, 2)
        def _(hh):
            pos = pl.multiple_of(first + hh * (second - first), half)
            slot = lax.div(pos, half)
            at = pl.ds(pos, half)
            out = pl.ds(pl.multiple_of(hh * half, half), half)
            cos_a = tab_ref[pl.ds(slot, 1), :]
            sin_a = tab_ref[pl.ds(n_slots + slot, 1), :]
            base = 2 * n_slots
            cos_o, sin_o, cos_n, sin_n = (tab_ref[base + n * half:base + (n + 1) * half, :] for n in range(4))
            cos_b = cos_a * cos_o - sin_a * sin_o
            sin_b = sin_a * cos_n + cos_a * sin_n

            def rope(n):
                part = proj[out, n * hd:(n + 1) * hd]
                return (part * cos_b + pltpu.roll(part, hd // 2, 1) * sin_b).astype(BF16)

            for h in range(group):
                q_s[slot, h * half:(h + 1) * half, :] = rope(h)
            k_s[at, :] = rope(group)
            v_s[at, :] = proj[out, (group + 1) * hd:].astype(BF16)

    scale = math.log2(math.e) / math.sqrt(hd)

    def scores(q, start_key):
        keys = k_s[pl.ds(start_key, chunk), :]
        return lax.dot_general(q, keys, (((1,), (1,)), ((), ())), preferred_element_type=F32)

    def fold(s, op):
        out = s[:, :hd]
        for n in range(1, chunk // hd):
            out = op(out, s[:, n * hd:(n + 1) * hd])
        return out

    def attend(pos, out_row):
        q = q_s[lax.div(pos, half)]
        n_full = lax.div(pos, chunk)
        edge = pl.multiple_of(n_full * chunk, chunk)
        s = scores(q, edge)
        shape = (half, chunk)
        row = lax.broadcasted_iota(jnp.int32, shape, 0) + (pos - edge)
        keep = lax.broadcasted_iota(jnp.int32, shape, 1) <= row
        keep = jnp.concatenate([keep] * group, axis=0)
        s = jnp.where(keep, s, -jnp.inf)
        sc[n_full] = s
        l_s[...] = fold(s, jnp.maximum)

        @pl.loop(0, n_full)
        def _(c):
            s = scores(q, pl.multiple_of(c * chunk, chunk))
            sc[c] = s
            l_s[...] = jnp.maximum(l_s[...], fold(s, jnp.maximum))

        top = jnp.max(l_s[...], axis=1, keepdims=True)
        l_s[...] = jnp.zeros_like(l_s)
        ctx_acc[...] = jnp.zeros_like(ctx_acc)

        @pl.loop(0, n_full + 1)
        def _(c):
            p = jnp.exp2((sc[c] - top) * scale)
            l_s[...] += fold(p, jnp.add)
            ctx_acc[...] += dot(p.astype(BF16), v_s[pl.ds(pl.multiple_of(c * chunk, chunk), chunk), :])

        out = (ctx_acc[...] / jnp.sum(l_s[...], axis=1, keepdims=True)).astype(BF16)
        for h in range(group):
            c_s[pl.ds(out_row, half), h * hd:(h + 1) * hd] = out[h * half:(h + 1) * half, :]

    def tile(j, emit):
        first, second = halves(j)

        @pl.loop(0, 2)
        def _(hh):
            attend(pl.multiple_of(first + hh * (second - first), half), pl.multiple_of(hh * half, half))

        project(c_s, wo, 1024, emit)

    for load in loads:
        load.wait()
    qkv(0)
    arrived(copies, 'd1')
    qkv(1)
    arrived(copies, 'xh0', 'yh1')
    start(copies, 'xf', 'yf', 'd2', 'xh1', 'yh0')
    qkv(3)
    arrived(copies, 'd2')
    qkv(2)
    arrived(copies, 'xf', 'yf')
    start(copies, 'd4')
    qkv(5)
    arrived(copies, 'd4')
    qkv(4)
    arrived(copies, 'xh1', 'yh0')
    start(copies, 'd6')
    qkv(7)
    arrived(copies, 'd6')
    qkv(6)

    tile(2, to_partner(2))
    start(copies, 'p2')
    arrived(copies, 'p2')
    tile(3, chip_sum(1, 0))
    start(copies, 'X0', 'Y1')
    tile(4, to_partner(4))
    start(copies, 'p4')
    arrived(copies, 'p4')
    tile(5, chip_sum(2, 1))
    start(copies, 'D0', 'D1')
    tile(6, to_partner(6))
    start(copies, 'p6')
    arrived(copies, 'p6')
    tile(7, last)
    tile(1, to_partner(1))
    start(copies, 'p1')
    merge_last(copies, acc7, RD, S)
    tile(0, own)
    finish(copies, r_ref, acc0, PR, RX, RY, o_ref)


def comm_scratch(rows, width):
    return [
        pltpu.VMEM((8, rows, width), BF16),
        pltpu.VMEM((4, rows, width), BF16),
        pltpu.VMEM((rows, width), BF16),
        pltpu.VMEM((rows, width), BF16),
        pltpu.VMEM((rows, width), BF16),
        pltpu.VMEM((3, rows, width), BF16),
        pltpu.VMEM((rows, width), F32),
        pltpu.VMEM((rows, width), F32),
    ]


def semaphores(n_loads):
    return [pltpu.SemaphoreType.DMA((N_COPIES,)), pltpu.SemaphoreType.DMA((N_COPIES,)),
            pltpu.SemaphoreType.DMA((n_loads,))]


def call(kernel, collective, out_dtype, rows, width, n_vmem, n_any, scratch, name):
    vmem = pl.BlockSpec(memory_space=pltpu.VMEM)
    return pl.pallas_call(
        kernel,
        out_shape=jax.ShapeDtypeStruct((rows, width), out_dtype),
        in_specs=[vmem] * n_vmem + [pl.BlockSpec(memory_space=pl.ANY)] * n_any,
        out_specs=vmem,
        scratch_shapes=scratch,
        compiler_params=pltpu.CompilerParams(
            collective_id=collective, has_side_effects=True, vmem_limit_bytes=VMEM_LIMIT),
        name=name,
    )


def rope_tables(seq_len, hd, half):
    inv_freq = ROPE_BASE ** (-2.0 * np.arange(hd // 2) / hd)
    inv_freq = np.concatenate([inv_freq, inv_freq])[None, :]
    slots = half * np.arange(seq_len // half)[:, None] * inv_freq
    offs = np.arange(half)[:, None] * inv_freq
    sign = np.where(np.arange(hd) < hd // 2, -1.0, 1.0)[None, :]
    rows = [np.cos(slots), np.sin(slots), np.cos(offs), np.sin(offs), sign * np.cos(offs), sign * np.sin(offs)]
    return np.concatenate(rows).astype(np.float32)


def solution(mesh):
    n_tp = mesh.shape['tp']
    tok_spec = P('dp', 'tp', None)
    in_specs = (tok_spec, P(), P(None, None, 'tp', None), P(), P(None, 'tp', None, None), P(), P(None, None, 'tp'), P(None, None, 'tp'), P(None, 'tp', None))

    def body(hidden, norm_attn, w_q, w_kv, w_o, norm_mlp, w_gate, w_up, w_down):
        n_layers, width, heads_loc, hd = w_q.shape
        rows = hidden.shape[1]
        seq_len = rows * n_tp
        half = rows // 2
        ff = w_gate.shape[2]
        n_kv = w_kv.shape[3]
        chunk = 512
        kv_rows = 256 * 2 * n_kv
        wq = jnp.transpose(w_q, (0, 2, 1, 3))
        wkv = w_kv.reshape(n_layers, width * 2 * n_kv, hd)
        wo = w_o.reshape(n_layers, heads_loc * hd, width)
        tab = jnp.asarray(rope_tables(seq_len, hd, half))
        attn_scratch = [
            pltpu.VMEM((width, (heads_loc + 2) * hd), BF16), pltpu.VMEM(wo.shape[1:], BF16), *comm_scratch(rows, width),
            pltpu.VMEM((seq_len // half, heads_loc * half, hd), BF16),
            pltpu.VMEM((seq_len, hd), BF16), pltpu.VMEM((seq_len, hd), BF16),
            pltpu.VMEM((seq_len // chunk, heads_loc * half, chunk), F32),
            pltpu.VMEM((heads_loc * half, hd), F32), pltpu.VMEM((heads_loc * half, hd), F32),
            pltpu.VMEM((rows, heads_loc * hd), BF16), pltpu.VMEM((rows, (heads_loc + 2) * hd), F32),
            pltpu.VMEM((2, kv_rows, hd), BF16), pltpu.VMEM((kv_rows, hd), F32), *semaphores(3 + heads_loc)]
        mlp_scratch = [
            pltpu.VMEM((width, ff), BF16), pltpu.VMEM((width, ff), BF16), pltpu.VMEM((ff, width), BF16),
            *comm_scratch(rows, width), pltpu.VMEM((2, rows, ff), BF16), *semaphores(3)]
        resid = hidden[0]
        for layer in range(n_layers):
            out_dtype = BF16 if layer == n_layers - 1 else F32
            resid = call(functools.partial(attn_kernel, layer, hd, n_kv), 2 * layer, F32, rows, width, 3, 3, attn_scratch, f'attn{layer}')(
                resid, norm_attn, tab, wq, wkv, wo)
            resid = call(functools.partial(mlp_kernel, layer), 2 * layer + 1, out_dtype, rows, width, 2, 3, mlp_scratch, f'mlp{layer}')(
                resid, norm_mlp, w_gate, w_up, w_down)
        return resid[None]

    return jax.shard_map(body, mesh=mesh, in_specs=in_specs, out_specs=tok_spec, check_vma=False)
```

```python
import functools
import math
import jax
import numpy as np
import jax.numpy as jnp
from jax import lax
from jax.experimental import pallas as pl
from jax.experimental.pallas import tpu as pltpu
from jax.sharding import PartitionSpec as P

EPS = 1e-5
ROPE_BASE = 10000.0
MESH = pl.DeviceIdType.MESH
VMEM_LIMIT = 67043328
F32 = jnp.float32
BF16 = jnp.bfloat16
N_COPIES = 20


def dot(a, b):
    return jnp.dot(a, b, preferred_element_type=F32)


def places():
    me = lax.axis_index('tp')
    core = lax.rem(me, 2)
    x = lax.rem(lax.div(me, 2), 2)
    y = lax.div(me, 4)
    dx = 2 - 4 * x
    dy = 4 - 8 * y
    return me, me + 1 - 2 * core, dx, dy


def greet(pa, xn, yn):
    for dev in (pa, xn, yn):
        pl.semaphore_signal(pltpu.get_barrier_semaphore(), inc=1, device_id={'tp': dev}, device_id_type=MESH)


def all_entered():
    pl.semaphore_wait(pltpu.get_barrier_semaphore(), 3)


def make_copies(G, PR, RX, RY, RD, S, ss, rs, pa, xn, yn):
    half = G.shape[1] // 2
    lo, hi = pl.ds(0, half), pl.ds(half, half)
    table = {
        'd0': (G.at[0], G.at[1], pa),
        'xh0': (G.at[0, lo], G.at[2, lo], xn),
        'yh1': (G.at[0, hi], G.at[2, hi], yn),
        'xf': (G.at[2, hi], G.at[6, hi], xn),
        'yf': (G.at[2, lo], G.at[6, lo], yn),
        'xh1': (G.at[0, hi], G.at[4, lo], xn),
        'yh0': (G.at[0, lo], G.at[4, hi], yn),
        'd2': (G.at[2], G.at[3], pa),
        'd4': (G.at[4], G.at[5], pa),
        'd6': (G.at[6], G.at[7], pa),
        'p1': (G.at[1], PR.at[0], pa),
        'p3': (G.at[3], PR.at[1], pa),
        'p5': (G.at[5], PR.at[3], pa),
        'p7': (G.at[7], PR.at[2], pa),
        'X0': (S.at[0, lo], RX.at[lo], xn),
        'Y1': (S.at[0, hi], RY.at[hi], yn),
        'D0': (S.at[1, lo], RD.at[hi], xn),
        'D1': (S.at[1, hi], RD.at[lo], yn),
        'X1': (S.at[2, lo], RX.at[hi], xn),
        'Y0': (S.at[2, hi], RY.at[lo], yn),
    }
    copies = {}
    for i, (name, (src, dst, dev)) in enumerate(table.items()):
        copies[name] = pltpu.make_async_remote_copy(
            src_ref=src, dst_ref=dst, send_sem=ss.at[i], recv_sem=rs.at[i],
            device_id={'tp': dev}, device_id_type=MESH)
    return copies


def start(copies, *names):
    for name in names:
        copies[name].start()


def arrived(copies, *names):
    for name in names:
        copies[name].wait_recv()


def norm_rows(layer, r_ref, g_ref, G):
    rows = r_ref.shape[0]
    step = 32

    @pl.loop(0, rows // step)
    def _(i):
        at = pl.ds(pl.multiple_of(i * step, step), step)
        x = r_ref[at, :].astype(F32)
        mean_sq = jnp.mean(x * x, axis=-1, keepdims=True)
        G[0, at, :] = (x * lax.rsqrt(mean_sq + EPS) * g_ref[layer:layer + 1, :]).astype(BF16)


def finish(copies, r_ref, acc0, PR, RX, RY, o_ref):
    arrived(copies, 'p1', 'X0', 'X1', 'Y0', 'Y1')
    rows = r_ref.shape[0]
    step = 32

    @pl.loop(0, rows // step)
    def _(i):
        at = pl.ds(pl.multiple_of(i * step, step), step)
        total = acc0[at, :] + PR[0, at, :].astype(F32)
        total += RX[at, :].astype(F32) + RY[at, :].astype(F32)
        o_ref[at, :] = (r_ref[at, :].astype(F32) + total).astype(o_ref.dtype)

    for copy in copies.values():
        copy.wait_send()


def project(a_ref, w_ref, width, emit):
    @pl.loop(0, w_ref.shape[1] // width)
    def _(n):
        cols = pl.ds(pl.multiple_of(n * width, width), width)
        emit(cols, dot(a_ref[...], w_ref[:, cols]))


def merge_last(copies, acc7, RD, S):
    arrived(copies, 'D0', 'D1')
    rows = acc7.shape[0]
    step = 32

    @pl.loop(0, rows // step)
    def _(i):
        at = pl.ds(pl.multiple_of(i * step, step), step)
        S[2, at, :] = (acc7[at, :] + RD[at, :].astype(F32)).astype(BF16)

    start(copies, 'X1', 'Y0')


def emitters(G, PR, S, acc0, acc7):
    def to_partner(j):
        def emit(cols, part):
            G[j, :, cols] = part.astype(BF16)
        return emit

    def chip_sum(i, slot):
        def emit(cols, part):
            S[slot, :, cols] = (part + PR[i, :, cols].astype(F32)).astype(BF16)
        return emit

    def own(cols, part):
        acc0[:, cols] = part

    def last(cols, part):
        acc7[:, cols] = part + PR[3, :, cols].astype(F32)

    return to_partner, chip_sum, own, last


def mlp_kernel(layer, r_ref, g_ref, wg_h, wu_h, wd_h, o_ref,
               wg, wu, wd, G, PR, RX, RY, RD, S, acc0, acc7, u, ss, rs, ls):
    me, pa, dx, dy = places()
    xn, yn = me + dx, me + dy
    greet(pa, xn, yn)
    loads = [pltpu.make_async_copy(h.at[layer], v, ls.at[i])
             for i, (h, v) in enumerate(((wg_h, wg), (wu_h, wu), (wd_h, wd)))]
    for load in loads:
        load.start()
    norm_rows(layer, r_ref, g_ref, G)
    all_entered()
    copies = make_copies(G, PR, RX, RY, RD, S, ss, rs, pa, xn, yn)
    to_partner, chip_sum, own, last = emitters(G, PR, S, acc0, acc7)
    start(copies, 'xh0', 'yh1', 'd0')

    def hidden(j):
        width = 256
        blocks = wg.shape[1] // width

        @pl.loop(0, 2 * blocks)
        def _(i):
            t = lax.div(i, blocks)
            cols = pl.ds(pl.multiple_of(lax.rem(i, blocks) * width, width), width)
            gate = dot(G[j + t], wg[:, cols])
            up = dot(G[j + t], wu[:, cols])
            u[t, :, cols] = (jax.nn.silu(gate) * up).astype(BF16)

    def down(t, emit):
        project(u.at[t], wd, 512, emit)

    for load in loads:
        load.wait()
    arrived(copies, 'd0')
    hidden(0)
    down(1, to_partner(1))
    start(copies, 'p1')
    arrived(copies, 'xh0', 'yh1')
    start(copies, 'xf', 'yf', 'd2', 'xh1', 'yh0')
    down(0, own)
    arrived(copies, 'd2')
    hidden(2)
    down(1, to_partner(3))
    start(copies, 'p3')
    arrived(copies, 'p3')
    down(0, chip_sum(1, 0))
    start(copies, 'X0', 'Y1')
    arrived(copies, 'xf', 'yf')
    start(copies, 'd6')
    arrived(copies, 'd6')
    hidden(6)
    down(1, to_partner(7))
    start(copies, 'p7')
    arrived(copies, 'p7')
    down(0, chip_sum(2, 1))
    start(copies, 'D0', 'D1')
    arrived(copies, 'xh1', 'yh0')
    start(copies, 'd4')
    arrived(copies, 'd4')
    hidden(4)
    down(1, to_partner(5))
    start(copies, 'p5')
    arrived(copies, 'p5')
    down(0, last)
    merge_last(copies, acc7, RD, S)
    finish(copies, r_ref, acc0, PR, RX, RY, o_ref)


def attn_kernel(layer, hd, n_kv, r_ref, g_ref, tab_ref, wq_h, wkv_h, wo_h, o_ref,
                wqkv, wo, G, PR, RX, RY, RD, S, acc0, acc7, q_s, k_s, v_s, top_s, sum_s, ctx_s, c_s,
                proj, kv_in, kv_f, ss, rs, ls):
    me, pa, dx, dy = places()
    xn, yn = me + dx, me + dy
    greet(pa, xn, yn)
    rows = r_ref.shape[0]
    half = rows // 2
    group = wo.shape[0] // hd
    chunk = 2 * rows
    n_slots = q_s.shape[0]
    kv_rows = kv_in.shape[1]
    depth = kv_rows // (2 * n_kv)
    n_parts = wqkv.shape[0] // depth

    def kv_load(i, slot):
        at = pl.ds(pl.multiple_of(i * kv_rows, kv_rows), kv_rows)
        return pltpu.make_async_copy(wkv_h.at[layer, at], kv_in.at[slot], ls.at[slot])

    kv_load(0, 0).start()
    loads = [pltpu.make_async_copy(wq_h.at[layer, h], wqkv.at[:, h * hd:(h + 1) * hd], ls.at[3 + h])
             for h in range(group)]
    loads.append(pltpu.make_async_copy(wo_h.at[layer], wo, ls.at[2]))
    for load in loads:
        load.start()
    norm_rows(layer, r_ref, g_ref, G)
    all_entered()
    copies = make_copies(G, PR, RX, RY, RD, S, ss, rs, pa, xn, yn)
    to_partner, chip_sum, own, last = emitters(G, PR, S, acc0, acc7)
    start(copies, 'xh0', 'yh1', 'd0', 'xh1', 'yh0')

    @pl.loop(0, n_parts)
    def _(i):
        slot = lax.rem(i, 2)

        @pl.when(i + 1 < n_parts)
        def _():
            kv_load(i + 1, 1 - slot).start()

        kv_load(i, slot).wait()
        piece = 512

        @pl.loop(0, kv_rows // piece)
        def _(n):
            at = pl.ds(pl.multiple_of(n * piece, piece), piece)
            kv_f[at, :] = kv_in[slot, at, :].astype(F32)

        at = pl.ds(pl.multiple_of(i * depth, depth), depth)
        for c in range(2):
            picked = kv_f[pl.ds(me + c * n_kv, depth, stride=2 * n_kv), :]
            wqkv[at, (group + c) * hd:(group + c + 1) * hd] = picked.astype(BF16)

    def position(i, t, hh):
        dev = me + t * (pa - me)
        far, diag = lax.div(i + 2, 3), lax.div(i, 3)
        swap = lax.div(i, 2) - diag
        first = (dev + far * dx + diag * dy) * rows + swap * half
        second = (dev + far * dy + diag * dx) * rows + (1 - swap) * half
        return pl.multiple_of(first + hh * (second - first), half)

    def qkv(i, t):
        proj[...] = dot(G[2 * i + t], wqkv[...])

        @pl.loop(0, 2)
        def _(hh):
            pos = position(i, t, hh)
            slot = lax.div(pos, half)
            at = pl.ds(pos, half)
            out = pl.ds(pl.multiple_of(hh * half, half), half)
            cos_a = tab_ref[pl.ds(slot, 1), :]
            sin_a = tab_ref[pl.ds(n_slots + slot, 1), :]
            base = 2 * n_slots
            cos_o, sin_o, cos_n, sin_n = (tab_ref[base + n * half:base + (n + 1) * half, :] for n in range(4))
            cos_b = cos_a * cos_o - sin_a * sin_o
            sin_b = sin_a * cos_n + cos_a * sin_n

            def rope(n):
                part = proj[out, n * hd:(n + 1) * hd]
                return (part * cos_b + pltpu.roll(part, hd // 2, 1) * sin_b).astype(BF16)

            for h in range(group):
                q_s[slot, h * half:(h + 1) * half, :] = rope(h)
            k_s[at, :] = rope(group)
            v_s[at, :] = proj[out, (group + 1) * hd:].astype(BF16)

    scale = math.log2(math.e) / math.sqrt(hd)

    def scores(q, keys):
        return lax.dot_general(q, k_s[keys, :], (((1,), (1,)), ((), ())), preferred_element_type=F32)

    def fold(s, op):
        out = s[:, :hd]
        for n in range(1, chunk // hd):
            out = op(out, s[:, n * hd:(n + 1) * hd])
        return out

    def reset(st):
        top_s[st] = jnp.full(top_s.shape[1:], -jnp.inf, F32)
        sum_s[st] = jnp.zeros(sum_s.shape[1:], F32)
        ctx_s[st] = jnp.zeros(ctx_s.shape[1:], F32)

    def absorb(st, pos, c):
        keys = pl.ds(pl.multiple_of(c * chunk, chunk), chunk)
        s = scores(q_s[lax.div(pos, half)], keys)
        shape = (half, chunk)
        row = lax.broadcasted_iota(jnp.int32, shape, 0) + (pos - c * chunk)
        keep = lax.broadcasted_iota(jnp.int32, shape, 1) <= row
        s = jnp.where(jnp.concatenate([keep] * group, axis=0), s, -jnp.inf)
        old = top_s[st]
        top = jnp.maximum(old, jnp.max(fold(s, jnp.maximum), axis=1, keepdims=True))
        top_s[st] = top
        shrink = jnp.exp2((old - top) * scale)
        p = jnp.exp2((s - top[:, :1]) * scale)
        sum_s[st] = sum_s[st] * shrink + fold(p, jnp.add)
        ctx_s[st] = ctx_s[st] * shrink + dot(p.astype(BF16), v_s[keys, :])

    def settle(st, hh):
        out = (ctx_s[st] / jnp.sum(sum_s[st], axis=1, keepdims=True)).astype(BF16)
        at = pl.ds(pl.multiple_of(hh * half, half), half)
        for h in range(group):
            c_s[at, h * hd:(h + 1) * hd] = out[h * half:(h + 1) * half, :]

    chip = lax.div(me, 2)
    dx_chip, dy_chip = lax.div(dx, 2), lax.div(dy, 2)

    def early():
        @pl.loop(0, 4)
        def _(st):
            pos = position(1, 1 - lax.div(st, 2), lax.rem(st, 2))
            reset(st)

            @pl.loop(0, 3)
            def _(n):
                c = chip + lax.rem(n, 2) * dx_chip + lax.div(n, 2) * dy_chip

                @pl.when(c <= lax.div(pos, chunk))
                def _():
                    absorb(st, pos, c)

    def emit_pair(n, name, emit_partner, emit_own):
        @pl.when(n == 0)
        def _():
            project(c_s, wo, 1024, emit_partner)
            start(copies, name)

        @pl.when(n == 1)
        def _():
            if emit_own is not own:
                arrived(copies, name)
            project(c_s, wo, 1024, emit_own)

    def first_pair(name, emit_partner, emit_own):
        @pl.loop(0, 2)
        def _(n):
            @pl.loop(0, 2)
            def _(hh):
                pos = position(1, 1 - n, hh)
                c = chip + dx_chip + dy_chip

                @pl.when(c <= lax.div(pos, chunk))
                def _():
                    absorb(2 * n + hh, pos, c)

                settle(2 * n + hh, hh)

            emit_pair(n, name, emit_partner, emit_own)

    def pair(i, name, emit_partner, emit_own):
        @pl.loop(0, 2)
        def _(n):
            @pl.loop(0, 2)
            def _(hh):
                pos = position(i, 1 - n, hh)
                reset(0)

                @pl.loop(0, lax.div(pos, chunk) + 1)
                def _(c):
                    absorb(0, pos, c)

                settle(0, hh)

            emit_pair(n, name, emit_partner, emit_own)

    for load in loads:
        load.wait()

    @pl.loop(0, 4)
    def _(i):
        @pl.when(i == 1)
        def _():
            arrived(copies, 'xh0', 'yh1')
            start(copies, 'xf', 'yf', 'd2')

        @pl.when(i == 2)
        def _():
            arrived(copies, 'xh1', 'yh0')
            start(copies, 'd4')

        @pl.when(i == 3)
        def _():
            early()
            arrived(copies, 'xf', 'yf')
            start(copies, 'd6')

        @pl.loop(0, 2)
        def _(t):
            for n, name in enumerate(('d0', 'd2', 'd4', 'd6')):
                @pl.when((t == 1) & (i == n))
                def _(name=name):
                    arrived(copies, name)

            qkv(i, t)

    first_pair('p3', to_partner(3), chip_sum(1, 0))
    start(copies, 'X0', 'Y1')
    pair(3, 'p7', to_partner(7), chip_sum(2, 1))
    start(copies, 'D0', 'D1')
    pair(2, 'p5', to_partner(5), last)
    pair(0, 'p1', to_partner(1), own)
    merge_last(copies, acc7, RD, S)
    finish(copies, r_ref, acc0, PR, RX, RY, o_ref)


def comm_scratch(rows, width):
    return [
        pltpu.VMEM((8, rows, width), BF16),
        pltpu.VMEM((4, rows, width), BF16),
        pltpu.VMEM((rows, width), BF16),
        pltpu.VMEM((rows, width), BF16),
        pltpu.VMEM((rows, width), BF16),
        pltpu.VMEM((3, rows, width), BF16),
        pltpu.VMEM((rows, width), F32),
        pltpu.VMEM((rows, width), F32),
    ]


def semaphores(n_loads):
    return [pltpu.SemaphoreType.DMA((N_COPIES,)), pltpu.SemaphoreType.DMA((N_COPIES,)),
            pltpu.SemaphoreType.DMA((n_loads,))]


def call(kernel, collective, out_dtype, rows, width, n_vmem, n_any, scratch, name):
    vmem = pl.BlockSpec(memory_space=pltpu.VMEM)
    return pl.pallas_call(
        kernel,
        out_shape=jax.ShapeDtypeStruct((rows, width), out_dtype),
        in_specs=[vmem] * n_vmem + [pl.BlockSpec(memory_space=pl.ANY)] * n_any,
        out_specs=vmem,
        scratch_shapes=scratch,
        compiler_params=pltpu.CompilerParams(
            collective_id=collective, has_side_effects=True, vmem_limit_bytes=VMEM_LIMIT),
        name=name,
    )


def rope_tables(seq_len, hd, half):
    inv_freq = ROPE_BASE ** (-2.0 * np.arange(hd // 2) / hd)
    inv_freq = np.concatenate([inv_freq, inv_freq])[None, :]
    slots = half * np.arange(seq_len // half)[:, None] * inv_freq
    offs = np.arange(half)[:, None] * inv_freq
    sign = np.where(np.arange(hd) < hd // 2, -1.0, 1.0)[None, :]
    rows = [np.cos(slots), np.sin(slots), np.cos(offs), np.sin(offs), sign * np.cos(offs), sign * np.sin(offs)]
    return np.concatenate(rows).astype(np.float32)


def solution(mesh):
    n_tp = mesh.shape['tp']
    tok_spec = P('dp', 'tp', None)
    in_specs = (tok_spec, P(), P(None, None, 'tp', None), P(), P(None, 'tp', None, None), P(), P(None, None, 'tp'), P(None, None, 'tp'), P(None, 'tp', None))

    def body(hidden, norm_attn, w_q, w_kv, w_o, norm_mlp, w_gate, w_up, w_down):
        n_layers, width, heads_loc, hd = w_q.shape
        rows = hidden.shape[1]
        seq_len = rows * n_tp
        half = rows // 2
        ff = w_gate.shape[2]
        n_kv = w_kv.shape[3]
        kv_rows = 256 * 2 * n_kv
        wq = jnp.transpose(w_q, (0, 2, 1, 3))
        wkv = w_kv.reshape(n_layers, width * 2 * n_kv, hd)
        wo = w_o.reshape(n_layers, heads_loc * hd, width)
        tab = jnp.asarray(rope_tables(seq_len, hd, half))
        attn_scratch = [
            pltpu.VMEM((width, (heads_loc + 2) * hd), BF16), pltpu.VMEM(wo.shape[1:], BF16), *comm_scratch(rows, width),
            pltpu.VMEM((seq_len // half, heads_loc * half, hd), BF16),
            pltpu.VMEM((seq_len, hd), BF16), pltpu.VMEM((seq_len, hd), BF16),
            *[pltpu.VMEM((4, heads_loc * half, hd), F32)] * 3,
            pltpu.VMEM((rows, heads_loc * hd), BF16), pltpu.VMEM((rows, (heads_loc + 2) * hd), F32),
            pltpu.VMEM((2, kv_rows, hd), BF16), pltpu.VMEM((kv_rows, hd), F32), *semaphores(3 + heads_loc)]
        mlp_scratch = [
            pltpu.VMEM((width, ff), BF16), pltpu.VMEM((width, ff), BF16), pltpu.VMEM((ff, width), BF16),
            *comm_scratch(rows, width), pltpu.VMEM((2, rows, ff), BF16), *semaphores(3)]
        resid = hidden[0]
        for layer in range(n_layers):
            out_dtype = BF16 if layer == n_layers - 1 else F32
            resid = call(functools.partial(attn_kernel, layer, hd, n_kv), 2 * layer, F32, rows, width, 3, 3, attn_scratch, f'attn{layer}')(
                resid, norm_attn, tab, wq, wkv, wo)
            resid = call(functools.partial(mlp_kernel, layer), 2 * layer + 1, out_dtype, rows, width, 2, 3, mlp_scratch, f'mlp{layer}')(
                resid, norm_mlp, w_gate, w_up, w_down)
        return resid[None]

    return jax.shard_map(body, mesh=mesh, in_specs=in_specs, out_specs=tok_spec, check_vma=False)
```

```python
import functools
import math
import jax
import numpy as np
import jax.numpy as jnp
from jax import lax
from jax.experimental import pallas as pl
from jax.experimental.pallas import tpu as pltpu
from jax.sharding import PartitionSpec as P

EPS = 1e-5
ROPE_BASE = 10000.0
MESH = pl.DeviceIdType.MESH
VMEM_LIMIT = 67043328
F32 = jnp.float32
BF16 = jnp.bfloat16
N_COPIES = 20


def dot(a, b):
    return jnp.dot(a, b, preferred_element_type=F32)


def places():
    me = lax.axis_index('tp')
    core = lax.rem(me, 2)
    x = lax.rem(lax.div(me, 2), 2)
    y = lax.div(me, 4)
    dx = 2 - 4 * x
    dy = 4 - 8 * y
    return me, me + 1 - 2 * core, dx, dy


def greet(pa, xn, yn):
    for dev in (pa, xn, yn):
        pl.semaphore_signal(pltpu.get_barrier_semaphore(), inc=1, device_id={'tp': dev}, device_id_type=MESH)


def all_entered():
    pl.semaphore_wait(pltpu.get_barrier_semaphore(), 3)


def make_copies(G, PR, RX, RY, RD, S, ss, rs, pa, xn, yn):
    half = G.shape[1] // 2
    lo, hi = pl.ds(0, half), pl.ds(half, half)
    table = {
        'd0': (G.at[0], G.at[1], pa),
        'xh0': (G.at[0, lo], G.at[2, lo], xn),
        'yh1': (G.at[0, hi], G.at[2, hi], yn),
        'xf': (G.at[2, hi], G.at[6, hi], xn),
        'yf': (G.at[2, lo], G.at[6, lo], yn),
        'xh1': (G.at[0, hi], G.at[4, lo], xn),
        'yh0': (G.at[0, lo], G.at[4, hi], yn),
        'd2': (G.at[2], G.at[3], pa),
        'd4': (G.at[4], G.at[5], pa),
        'd6': (G.at[6], G.at[7], pa),
        'p1': (G.at[1], PR.at[0], pa),
        'p3': (G.at[3], PR.at[1], pa),
        'p5': (G.at[5], PR.at[3], pa),
        'p7': (G.at[7], PR.at[2], pa),
        'X0': (S.at[0, lo], RX.at[lo], xn),
        'Y1': (S.at[0, hi], RY.at[hi], yn),
        'D0': (S.at[1, lo], RD.at[hi], xn),
        'D1': (S.at[1, hi], RD.at[lo], yn),
        'X1': (S.at[2, lo], RX.at[hi], xn),
        'Y0': (S.at[2, hi], RY.at[lo], yn),
    }
    copies = {}
    for i, (name, (src, dst, dev)) in enumerate(table.items()):
        copies[name] = pltpu.make_async_remote_copy(
            src_ref=src, dst_ref=dst, send_sem=ss.at[i], recv_sem=rs.at[i],
            device_id={'tp': dev}, device_id_type=MESH)
    return copies


def start(copies, *names):
    for name in names:
        copies[name].start()


def arrived(copies, *names):
    for name in names:
        copies[name].wait_recv()


def normed(x, gain):
    mean_sq = jnp.mean(x * x, axis=-1, keepdims=True)
    return (x * lax.rsqrt(mean_sq + EPS) * gain).astype(BF16)


def norm_rows(r_s, gain_ref, G):
    step = 32

    @pl.loop(0, r_s.shape[0] // step)
    def _(i):
        at = pl.ds(pl.multiple_of(i * step, step), step)
        G[0, at, :] = normed(r_s[at, :].astype(F32), gain_ref[...])


def finish(copies, r_s, acc0, PR, RX, RY, o_ref, next_ref, gain_ref):
    arrived(copies, 'p1', 'X0', 'X1', 'Y0', 'Y1')
    step = 32

    @pl.loop(0, r_s.shape[0] // step)
    def _(i):
        at = pl.ds(pl.multiple_of(i * step, step), step)
        total = acc0[at, :] + PR[0, at, :].astype(F32)
        total += RX[at, :].astype(F32) + RY[at, :].astype(F32)
        x = r_s[at, :].astype(F32) + total
        o_ref[at, :] = x.astype(o_ref.dtype)
        if next_ref is not None:
            next_ref[at, :] = normed(x, gain_ref[...])

    for copy in copies.values():
        copy.wait_send()


def project(a_ref, w_ref, width, emit):
    @pl.loop(0, w_ref.shape[1] // width)
    def _(n):
        cols = pl.ds(pl.multiple_of(n * width, width), width)
        emit(cols, dot(a_ref[...], w_ref[:, cols]))


def merge_last(copies, acc7, RD, S):
    arrived(copies, 'D0', 'D1')
    rows = acc7.shape[0]
    step = 32

    @pl.loop(0, rows // step)
    def _(i):
        at = pl.ds(pl.multiple_of(i * step, step), step)
        S[2, at, :] = (acc7[at, :] + RD[at, :].astype(F32)).astype(BF16)

    start(copies, 'X1', 'Y0')


def emitters(G, PR, S, acc0, acc7):
    def to_partner(j):
        def emit(cols, part):
            G[j, :, cols] = part.astype(BF16)
        return emit

    def chip_sum(i, slot):
        def emit(cols, part):
            S[slot, :, cols] = (part + PR[i, :, cols].astype(F32)).astype(BF16)
        return emit

    def own(cols, part):
        acc0[:, cols] = part

    def last(cols, part):
        acc7[:, cols] = part + PR[3, :, cols].astype(F32)

    return to_partner, chip_sum, own, last


def mlp_kernel(layer, last_layer, r_h, a_h, na_ref, nm_ref, wg_h, wu_h, wd_h, o_ref, *refs):
    if last_layer:
        next_ref, gain_ref, acc0 = None, None, refs[-1]
        refs = refs[:-1]
    else:
        next_ref, gain_ref, acc0 = refs[0], na_ref.at[layer + 1:layer + 2], o_ref
        refs = refs[1:]
    wg, wu, wd, u, r_s, G, PR, RX, RY, RD, S, acc7, ss, rs, ls = refs
    me, pa, dx, dy = places()
    xn, yn = me + dx, me + dy
    greet(pa, xn, yn)
    loads = [pltpu.make_async_copy(h.at[layer], v, ls.at[i])
             for i, (h, v) in enumerate(((wg_h, wg), (wu_h, wu), (wd_h, wd)))]
    rows_in = pltpu.make_async_copy(a_h, G.at[0], ls.at[3])
    resid_in = pltpu.make_async_copy(r_h, r_s, ls.at[4])
    rows_in.start()
    rows_in.wait()
    all_entered()
    copies = make_copies(G, PR, RX, RY, RD, S, ss, rs, pa, xn, yn)
    to_partner, chip_sum, own, last = emitters(G, PR, S, acc0, acc7)
    start(copies, 'xh0', 'yh1', 'd0')
    for load in loads:
        load.start()
    resid_in.start()

    def hidden(j):
        width = 256
        blocks = wg.shape[1] // width

        @pl.loop(0, 2 * blocks)
        def _(i):
            t = lax.div(i, blocks)
            cols = pl.ds(pl.multiple_of(lax.rem(i, blocks) * width, width), width)
            gate = dot(G[j + t], wg[:, cols])
            up = dot(G[j + t], wu[:, cols])
            u[t, :, cols] = (jax.nn.silu(gate) * up).astype(BF16)

    def down(t, emit):
        project(u.at[t], wd, 512, emit)

    for load in loads:
        load.wait()
    arrived(copies, 'd0')
    hidden(0)
    down(1, to_partner(1))
    start(copies, 'p1')
    arrived(copies, 'xh0', 'yh1')
    start(copies, 'xf', 'yf', 'd2', 'xh1', 'yh0')
    down(0, own)
    arrived(copies, 'd2')
    hidden(2)
    down(1, to_partner(3))
    start(copies, 'p3')
    arrived(copies, 'p3')
    down(0, chip_sum(1, 0))
    start(copies, 'X0', 'Y1')
    arrived(copies, 'xf', 'yf')
    start(copies, 'd6')
    arrived(copies, 'd6')
    hidden(6)
    down(1, to_partner(7))
    start(copies, 'p7')
    arrived(copies, 'p7')
    down(0, chip_sum(2, 1))
    start(copies, 'D0', 'D1')
    arrived(copies, 'xh1', 'yh0')
    start(copies, 'd4')
    arrived(copies, 'd4')
    hidden(4)
    down(1, to_partner(5))
    start(copies, 'p5')
    arrived(copies, 'p5')
    down(0, last)
    merge_last(copies, acc7, RD, S)
    resid_in.wait()
    finish(copies, r_s, acc0, PR, RX, RY, o_ref, next_ref, gain_ref)


def attn_kernel(layer, hd, n_kv, r_h, a_h, na_ref, nm_ref, tab_ref, wq_h, wkv_h, wo_h, o_ref, next_ref,
                wqkv, wo, q_s, k_s, v_s, top_s, sum_s, ctx_s, c_s, proj, kv_in, kv_f,
                r_s, G, PR, RX, RY, RD, S, acc7, ss, rs, ls):
    acc0 = o_ref
    me, pa, dx, dy = places()
    xn, yn = me + dx, me + dy
    greet(pa, xn, yn)
    rows = r_s.shape[0]
    half = rows // 2
    group = wo.shape[0] // hd
    chunk = 2 * rows
    n_slots = q_s.shape[0]
    kv_rows = kv_in.shape[1]
    depth = kv_rows // (2 * n_kv)
    n_parts = wqkv.shape[0] // depth

    def kv_load(i, slot):
        at = pl.ds(pl.multiple_of(i * kv_rows, kv_rows), kv_rows)
        return pltpu.make_async_copy(wkv_h.at[layer, at], kv_in.at[slot], ls.at[slot])

    resid_in = pltpu.make_async_copy(r_h, r_s, ls.at[3 + group])
    rows_in = resid_in
    if layer > 0:
        rows_in = pltpu.make_async_copy(a_h, G.at[0], ls.at[4 + group])
    rows_in.start()
    loads = [pltpu.make_async_copy(wq_h.at[layer, h], wqkv.at[:, h * hd:(h + 1) * hd], ls.at[3 + h])
             for h in range(group)]
    loads.append(pltpu.make_async_copy(wo_h.at[layer], wo, ls.at[2]))
    rows_in.wait()
    if layer == 0:
        norm_rows(r_s, na_ref.at[layer:layer + 1], G)
    all_entered()
    copies = make_copies(G, PR, RX, RY, RD, S, ss, rs, pa, xn, yn)
    to_partner, chip_sum, own, last = emitters(G, PR, S, acc0, acc7)
    start(copies, 'xh0', 'yh1', 'd0', 'xh1', 'yh0')
    kv_load(0, 0).start()
    for load in loads:
        load.start()
    if layer > 0:
        resid_in.start()

    @pl.loop(0, n_parts)
    def _(i):
        slot = lax.rem(i, 2)

        @pl.when(i + 1 < n_parts)
        def _():
            kv_load(i + 1, 1 - slot).start()

        kv_load(i, slot).wait()
        piece = 512

        @pl.loop(0, kv_rows // piece)
        def _(n):
            at = pl.ds(pl.multiple_of(n * piece, piece), piece)
            kv_f[at, :] = kv_in[slot, at, :].astype(F32)

        at = pl.ds(pl.multiple_of(i * depth, depth), depth)
        for c in range(2):
            picked = kv_f[pl.ds(me + c * n_kv, depth, stride=2 * n_kv), :]
            wqkv[at, (group + c) * hd:(group + c + 1) * hd] = picked.astype(BF16)

    def position(i, t, hh):
        dev = me + t * (pa - me)
        far, diag = lax.div(i + 2, 3), lax.div(i, 3)
        swap = lax.div(i, 2) - diag
        first = (dev + far * dx + diag * dy) * rows + swap * half
        second = (dev + far * dy + diag * dx) * rows + (1 - swap) * half
        return pl.multiple_of(first + hh * (second - first), half)

    def turn(part, slot):
        cos_a = tab_ref[pl.ds(slot, 1), :]
        sin_a = tab_ref[pl.ds(n_slots + slot, 1), :]
        base = 2 * n_slots
        cos_o, sin_o, cos_n, sin_n = (tab_ref[base + n * half:base + (n + 1) * half, :] for n in range(4))
        cos_b = cos_a * cos_o - sin_a * sin_o
        sin_b = sin_a * cos_n + cos_a * sin_n
        return (part * cos_b + pltpu.roll(part, hd // 2, 1) * sin_b).astype(BF16)

    q_cols, kv_cols = pl.ds(0, group * hd), pl.ds(group * hd, 2 * hd)

    def keys_values(i, t):
        proj[:, kv_cols] = dot(G[2 * i + t], wqkv[:, kv_cols])

        @pl.loop(0, 2)
        def _(hh):
            pos = position(i, t, hh)
            out = pl.ds(pl.multiple_of(hh * half, half), half)
            k_s[pl.ds(pos, half), :] = turn(proj[out, group * hd:(group + 1) * hd], lax.div(pos, half))
            v_s[pl.ds(pos, half), :] = proj[out, (group + 1) * hd:].astype(BF16)

    def queries(i, t):
        proj[:, q_cols] = dot(G[2 * i + t], wqkv[:, q_cols])

        @pl.loop(0, 2)
        def _(hh):
            slot = lax.div(position(i, t, hh), half)
            out = pl.ds(pl.multiple_of(hh * half, half), half)
            for h in range(group):
                q_s[slot, h * half:(h + 1) * half, :] = turn(proj[out, h * hd:(h + 1) * hd], slot)

    scale = math.log2(math.e) / math.sqrt(hd)

    def scores(q, keys):
        return lax.dot_general(q, k_s[keys, :], (((1,), (1,)), ((), ())), preferred_element_type=F32)

    def fold(s, op):
        out = s[:, :hd]
        for n in range(1, chunk // hd):
            out = op(out, s[:, n * hd:(n + 1) * hd])
        return out

    def reset(st):
        top_s[st] = jnp.full(top_s.shape[1:], -jnp.inf, F32)
        sum_s[st] = jnp.zeros(sum_s.shape[1:], F32)
        ctx_s[st] = jnp.zeros(ctx_s.shape[1:], F32)

    def absorb(st, pos, c):
        keys = pl.ds(pl.multiple_of(c * chunk, chunk), chunk)
        s = scores(q_s[lax.div(pos, half)], keys)
        shape = (half, chunk)
        row = lax.broadcasted_iota(jnp.int32, shape, 0) + (pos - c * chunk)
        keep = lax.broadcasted_iota(jnp.int32, shape, 1) <= row
        s = jnp.where(jnp.concatenate([keep] * group, axis=0), s, -jnp.inf)
        old = top_s[st]
        top = jnp.maximum(old, jnp.max(fold(s, jnp.maximum), axis=1, keepdims=True))
        top_s[st] = top
        shrink = jnp.exp2((old - top) * scale)
        p = jnp.exp2((s - top[:, :1]) * scale)
        sum_s[st] = sum_s[st] * shrink + fold(p, jnp.add)
        ctx_s[st] = ctx_s[st] * shrink + dot(p.astype(BF16), v_s[keys, :])

    def settle(st, hh):
        out = (ctx_s[st] / jnp.sum(sum_s[st], axis=1, keepdims=True)).astype(BF16)
        at = pl.ds(pl.multiple_of(hh * half, half), half)
        for h in range(group):
            c_s[at, h * hd:(h + 1) * hd] = out[h * half:(h + 1) * half, :]

    chip = lax.div(me, 2)
    dx_chip, dy_chip = lax.div(dx, 2), lax.div(dy, 2)

    def early():
        @pl.loop(0, 4)
        def _(st):
            pos = position(1, 1 - lax.div(st, 2), lax.rem(st, 2))
            reset(st)

            @pl.loop(0, 3)
            def _(n):
                c = chip + lax.rem(n, 2) * dx_chip + lax.div(n, 2) * dy_chip

                @pl.when(c <= lax.div(pos, chunk))
                def _():
                    absorb(st, pos, c)

    def emit_pair(n, name, emit_partner, emit_own):
        @pl.when(n == 0)
        def _():
            project(c_s, wo, 1024, emit_partner)
            start(copies, name)

        @pl.when(n == 1)
        def _():
            if emit_own is not own:
                arrived(copies, name)
            project(c_s, wo, 1024, emit_own)

    def first_pair(name, emit_partner, emit_own):
        @pl.loop(0, 2)
        def _(n):
            @pl.loop(0, 2)
            def _(hh):
                pos = position(1, 1 - n, hh)
                c = chip + dx_chip + dy_chip

                @pl.when(c <= lax.div(pos, chunk))
                def _():
                    absorb(2 * n + hh, pos, c)

                settle(2 * n + hh, hh)

            emit_pair(n, name, emit_partner, emit_own)

    def pair(i, name, emit_partner, emit_own):
        @pl.loop(0, 2)
        def _(n):
            @pl.loop(0, 2)
            def _(hh):
                pos = position(i, 1 - n, hh)
                reset(0)

                @pl.loop(0, lax.div(pos, chunk) + 1)
                def _(c):
                    absorb(0, pos, c)

                settle(0, hh)

            emit_pair(n, name, emit_partner, emit_own)

    for load in loads:
        load.wait()

    @pl.loop(0, 4)
    def _(i):
        @pl.when(i == 1)
        def _():
            arrived(copies, 'xh0', 'yh1')
            start(copies, 'xf', 'yf', 'd2')

        @pl.when(i == 2)
        def _():
            arrived(copies, 'xh1', 'yh0')
            start(copies, 'd4')

        @pl.when(i == 3)
        def _():
            early()
            arrived(copies, 'xf', 'yf')
            start(copies, 'd6')

        @pl.loop(0, 2)
        def _(t):
            for n, name in enumerate(('d0', 'd2', 'd4', 'd6')):
                @pl.when((t == 1) & (i == n))
                def _(name=name):
                    arrived(copies, name)

            keys_values(i, t)

            @pl.when(i < 3)
            def _():
                queries(i, t)

    first_pair('p3', to_partner(3), chip_sum(1, 0))
    start(copies, 'X0', 'Y1')

    @pl.loop(0, 2)
    def _(t):
        queries(3, t)

    pair(3, 'p7', to_partner(7), chip_sum(2, 1))
    start(copies, 'D0', 'D1')
    pair(2, 'p5', to_partner(5), last)
    pair(0, 'p1', to_partner(1), own)
    merge_last(copies, acc7, RD, S)
    if layer > 0:
        resid_in.wait()
    finish(copies, r_s, acc0, PR, RX, RY, o_ref, next_ref, nm_ref.at[layer:layer + 1])


def comm_scratch(rows, width, n_loads, resid_dtype):
    return [
        pltpu.VMEM((rows, width), resid_dtype),
        pltpu.VMEM((8, rows, width), BF16),
        pltpu.VMEM((4, rows, width), BF16),
        pltpu.VMEM((rows, width), BF16),
        pltpu.VMEM((rows, width), BF16),
        pltpu.VMEM((rows, width), BF16),
        pltpu.VMEM((3, rows, width), BF16),
        pltpu.VMEM((rows, width), F32),
        pltpu.SemaphoreType.DMA((N_COPIES,)),
        pltpu.SemaphoreType.DMA((N_COPIES,)),
        pltpu.SemaphoreType.DMA((n_loads,)),
    ]


def call(kernel, collective, shapes, n_vmem, n_any, scratch, name):
    vmem, anywhere = pl.BlockSpec(memory_space=pltpu.VMEM), pl.BlockSpec(memory_space=pl.ANY)
    return pl.pallas_call(
        kernel,
        out_shape=shapes,
        in_specs=[anywhere] * 2 + [vmem] * n_vmem + [anywhere] * n_any,
        out_specs=[vmem] * len(shapes),
        scratch_shapes=scratch,
        compiler_params=pltpu.CompilerParams(
            collective_id=collective, has_side_effects=True, vmem_limit_bytes=VMEM_LIMIT),
        name=name,
    )


def rope_tables(seq_len, hd, half):
    inv_freq = ROPE_BASE ** (-2.0 * np.arange(hd // 2) / hd)
    inv_freq = np.concatenate([inv_freq, inv_freq])[None, :]
    slots = half * np.arange(seq_len // half)[:, None] * inv_freq
    offs = np.arange(half)[:, None] * inv_freq
    sign = np.where(np.arange(hd) < hd // 2, -1.0, 1.0)[None, :]
    rows = [np.cos(slots), np.sin(slots), np.cos(offs), np.sin(offs), sign * np.cos(offs), sign * np.sin(offs)]
    return np.concatenate(rows).astype(np.float32)


def solution(mesh):
    n_tp = mesh.shape['tp']
    tok_spec = P('dp', 'tp', None)
    in_specs = (tok_spec, P(), P(None, None, 'tp', None), P(), P(None, 'tp', None, None), P(), P(None, None, 'tp'), P(None, None, 'tp'), P(None, 'tp', None))

    def body(hidden, norm_attn, w_q, w_kv, w_o, norm_mlp, w_gate, w_up, w_down):
        n_layers, width, heads_loc, hd = w_q.shape
        rows = hidden.shape[1]
        seq_len = rows * n_tp
        half = rows // 2
        ff = w_gate.shape[2]
        n_kv = w_kv.shape[3]
        kv_rows = 256 * 2 * n_kv
        wq = jnp.transpose(w_q, (0, 2, 1, 3))
        wkv = w_kv.reshape(n_layers, width * 2 * n_kv, hd)
        wo = w_o.reshape(n_layers, heads_loc * hd, width)
        tab = jnp.asarray(rope_tables(seq_len, hd, half))
        attn_scratch = [
            pltpu.VMEM((width, (heads_loc + 2) * hd), BF16), pltpu.VMEM(wo.shape[1:], BF16),
            pltpu.VMEM((seq_len // half, heads_loc * half, hd), BF16),
            pltpu.VMEM((seq_len, hd), BF16), pltpu.VMEM((seq_len, hd), BF16),
            *[pltpu.VMEM((4, heads_loc * half, hd), F32)] * 3,
            pltpu.VMEM((rows, heads_loc * hd), BF16), pltpu.VMEM((rows, (heads_loc + 2) * hd), F32),
            pltpu.VMEM((2, kv_rows, hd), BF16), pltpu.VMEM((kv_rows, hd), F32)]
        mlp_scratch = [
            pltpu.VMEM((width, ff), BF16), pltpu.VMEM((width, ff), BF16), pltpu.VMEM((ff, width), BF16),
            pltpu.VMEM((2, rows, ff), BF16), *comm_scratch(rows, width, 5, F32)]
        both = [jax.ShapeDtypeStruct((rows, width), F32), jax.ShapeDtypeStruct((rows, width), BF16)]
        resid = following = hidden[0]
        for layer in range(n_layers):
            last_layer = layer == n_layers - 1
            resid, following = call(
                functools.partial(attn_kernel, layer, hd, n_kv), 2 * layer, both, 3, 3,
                attn_scratch + comm_scratch(rows, width, 5 + heads_loc, resid.dtype), f'attn{layer}')(
                resid, following, norm_attn, norm_mlp, tab, wq, wkv, wo)
            resid, *following = call(
                functools.partial(mlp_kernel, layer, last_layer), 2 * layer + 1, both[1:] if last_layer else both, 2, 3,
                mlp_scratch + [pltpu.VMEM((rows, width), F32)] * last_layer, f'mlp{layer}')(
                resid, following, norm_attn, norm_mlp, w_gate, w_up, w_down)
            following = following[0] if following else None
        return resid[None]

    return jax.shard_map(body, mesh=mesh, in_specs=in_specs, out_specs=tok_spec, check_vma=False)
```
